32 devices in a mesh: limb: 4 (over z), coef: 8 (over y, x, core).
Axes of the slice: x: 2, y: 2, z: 4, core: 2. Of those that a mesh axis runs over, the one named last changes fastest.
Arguments:
- cipher_zero: float32 [24, 32, 65536], P(None, 'limb', 'coef'), may hold values from -6 to 6
- cipher_one: float32 [24, 32, 65536], P(None, 'limb', 'coef'), may hold values from -6 to 6
- key_main: bfloat16 [24, 2, 2, 32, 65536], P(None, None, None, 'limb', 'coef'), may hold values from -5 to 5
- key_special: bfloat16 [24, 2, 2, 16, 65536], P(None, None, None, 'limb', 'coef'), may hold values from -5 to 5
- lift_main: float32 [32, 32], replicated, may hold values from -1.5 to 1.5
- lift_special: float32 [32, 16], replicated, may hold values from -1.5 to 1.5
- lower_table: float32 [16, 32], replicated, may hold values from -1.5 to 1.5
- inverse_scale: float32 [32], P('limb'), may hold values from 0.5 to 1.5
- inverse_main: float32 [32, 256, 256], P('limb', 'coef'), may hold values from 0.5 to 1.5
- inverse_special: float32 [16, 256, 256], P('limb', 'coef'), may hold values from 0.5 to 1.5
- forward_main: float32 [32, 256, 256], P('limb', 'coef'), may hold values from 0.5 to 1.5
- forward_special: float32 [16, 256, 256], P('limb', 'coef'), may hold values from 0.5 to 1.5
- inverse_rows: float32 [256, 256], replicated, may hold values from -0.375 to 0.375
- inverse_columns: float32 [256, 256], replicated, may hold values from -0.375 to 0.375
- forward_rows: float32 [256, 256], replicated, may hold values from -0.375 to 0.375
- forward_columns: float32 [256, 256], replicated, may hold values from -0.375 to 0.375
Outputs:
- switched_zero: float32 [24, 32, 65536], P(None, 'limb', 'coef')
- switched_one: float32 [24, 32, 65536], P(None, 'limb', 'coef')
The draws below stay inside these ranges and needn't reach their ends.
All inputs are finite; a program needn't handle non-finite values.
Results may differ from the reference program's by a relative error of at most 0.0003.
Values sent between devices are 32-bit elements; how exact they have to be, the bound alone decides.
No kernel may reach another device: no remote copies, remote signals or barrier semaphores. Data moves between devices by JAX's collectives and lax.ppermute only.
A program may use at most 192 MiB of HBM per device.

```python
import jax
import jax.numpy as jnp
from jax import lax

CT = 24
L = 32
K = 16
ROWS = 256
COLS = 256
DIGITS = 2
N = 65536


def shard_levels(key, dims, pieces, least, high):
    factor_of, own = 1.0, jax.random.fold_in(key, 6)
    for dim, blocks in pieces:
        heights = jnp.exp(jax.random.uniform(jax.random.fold_in(own, dim), (blocks,), jnp.float32, least / len(pieces), high / len(pieces)))
        factor_of = factor_of * jnp.repeat(heights, dims[dim] // blocks).reshape([-1 if axis == dim else 1 for axis in range(len(dims))])
    return factor_of


def noise(key, shape, deviation, most, shards=(), kind=jnp.bfloat16):
    entries = jax.random.normal(key, shape, jnp.float32) * deviation
    if len(shards) > 0:
        entries = shard_levels(key, shape, shards, -0.22, 0.18) * entries
    return jnp.clip(entries, min=-most, max=most).astype(kind)


def setup_inputs(seed: int = 0) -> dict:
    seeds = jax.random.split(jax.random.key(seed), 17)
    return {
        "cipher_zero": noise(seeds[0], (CT, L, N), 1.0, 6.0, ((1, 4), (2, 8)), jnp.float32),
        "cipher_one": noise(seeds[1], (CT, L, N), 1.0, 6.0, ((1, 4), (2, 8)), jnp.float32),
        "key_main": noise(seeds[2], (CT, DIGITS, 2, L, N), 0.7, 5.0, ((3, 4), (4, 8))),
        "key_special": noise(seeds[3], (CT, DIGITS, 2, K, N), 0.7, 5.0, ((3, 4), (4, 8))),
        "lift_main": noise(seeds[4], (L, L), K ** -0.5, 1.5, (), jnp.float32),
        "lift_special": noise(seeds[5], (L, K), K ** -0.5, 1.5, (), jnp.float32),
        "lower_table": noise(seeds[6], (K, L), K ** -0.5, 1.5, (), jnp.float32),
        "inverse_scale": jnp.clip(0.5 + 1.0 * jax.random.uniform(seeds[7], (L,), jnp.float32) ** shard_levels(seeds[7], (L,), ((0, 4),), -0.2, 0.2), 0.5, 1.5),
        "inverse_main": jnp.clip(0.5 + 1.0 * jax.random.uniform(seeds[8], (L, ROWS, COLS), jnp.float32) ** shard_levels(seeds[8], (L, ROWS, COLS), ((0, 4), (1, 8)), -0.2, 0.2), 0.5, 1.5),
        "inverse_special": jnp.clip(0.5 + 1.0 * jax.random.uniform(seeds[9], (K, ROWS, COLS), jnp.float32) ** shard_levels(seeds[9], (K, ROWS, COLS), ((0, 4), (1, 8)), -0.2, 0.2), 0.5, 1.5),
        "forward_main": jnp.clip(0.5 + 1.0 * jax.random.uniform(seeds[10], (L, COLS, ROWS), jnp.float32) ** shard_levels(seeds[10], (L, COLS, ROWS), ((0, 4), (1, 8)), -0.2, 0.2), 0.5, 1.5),
        "forward_special": jnp.clip(0.5 + 1.0 * jax.random.uniform(seeds[11], (K, COLS, ROWS), jnp.float32) ** shard_levels(seeds[11], (K, COLS, ROWS), ((0, 4), (1, 8)), -0.2, 0.2), 0.5, 1.5),
        "inverse_rows": noise(seeds[12], (ROWS, ROWS), ROWS ** -0.5, 0.375, (), jnp.float32),
        "inverse_columns": noise(seeds[13], (COLS, COLS), COLS ** -0.5, 0.375, (), jnp.float32),
        "forward_rows": noise(seeds[14], (ROWS, ROWS), ROWS ** -0.5, 0.375, (), jnp.float32),
        "forward_columns": noise(seeds[15], (COLS, COLS), COLS ** -0.5, 0.375, (), jnp.float32),
    }


HIGHEST = lax.Precision.HIGHEST


def inverse_four(values, twiddle, inverse_rows, inverse_columns):
    partial_value = jnp.einsum("...rc,ck->...rk", values, inverse_columns, precision=HIGHEST) * twiddle
    return jnp.einsum("...rk,rj->...kj", partial_value, inverse_rows, precision=HIGHEST)


def forward_four(coeffs, twiddle, forward_rows, forward_columns):
    partial_value = jnp.einsum("...cr,rk->...ck", coeffs, forward_rows, precision=HIGHEST) * twiddle
    return jnp.einsum("...ck,cm->...km", partial_value, forward_columns, precision=HIGHEST)


def reference(cipher_zero, cipher_one, key_main, key_special, lift_main, lift_special, lower_table, inverse_scale, inverse_main, inverse_special, forward_main, forward_special, inverse_rows, inverse_columns, forward_rows, forward_columns):
    digits = L // K
    owner = (jnp.arange(L) // K)[None, :] == jnp.arange(digits)[:, None]
    digit_mask = owner.astype(lift_main.dtype)
    masked_main = digit_mask[:, :, None] * lift_main[None]
    masked_special = digit_mask[:, :, None] * lift_special[None]

    def single(record):
        first_part, second_part, keys_main, keys_special = record
        coeffs = inverse_four(second_part.reshape(L, ROWS, COLS), inverse_main, inverse_rows, inverse_columns).reshape(L, ROWS * COLS)
        lifted_main = jnp.einsum("sn,dst->dtn", coeffs, masked_main, precision=HIGHEST)
        lifted_sp = jnp.einsum("sn,dst->dtn", coeffs, masked_special, precision=HIGHEST)
        values_main = forward_four(lifted_main.reshape(digits, L, COLS, ROWS), forward_main, forward_rows, forward_columns).reshape(digits, L, ROWS * COLS)
        values_sp = forward_four(lifted_sp.reshape(digits, K, COLS, ROWS), forward_special, forward_rows, forward_columns).reshape(digits, K, ROWS * COLS)
        summed_main = jnp.sum(values_main[:, None] * keys_main.astype(values_main.dtype), axis=0)
        summed_sp = jnp.sum(values_sp[:, None] * keys_special.astype(values_sp.dtype), axis=0)
        special = inverse_four(summed_sp.reshape(2, K, ROWS, COLS), inverse_special, inverse_rows, inverse_columns).reshape(2, K, ROWS * COLS)
        lowered = jnp.einsum("sjn,jt->stn", special, lower_table, precision=HIGHEST)
        lowered = forward_four(lowered.reshape(2, L, COLS, ROWS), forward_main, forward_rows, forward_columns).reshape(2, L, ROWS * COLS)
        result = inverse_scale[:, None] * (summed_main - lowered)
        return first_part + result[0], result[1]

    switched_zero, switched_one = lax.map(single, (cipher_zero, cipher_one, key_main, key_special))
    return switched_zero, switched_one
```

```python
import functools

import jax
import jax.numpy as jnp
from jax import lax
from jax.experimental import pallas as pl
from jax.experimental.pallas import tpu as pltpu
from jax.sharding import PartitionSpec as P


K = 16
ROWS = 256
COLS = 256
SIZES = (2, 4, 4, 4, 4, 4, 2)
F32 = jnp.float32
BF16 = jnp.bfloat16


HIGHEST = lax.Precision.HIGHEST


def columns_section(values, twiddle, inverse_columns):
    partial_value = (
        jnp.einsum("...rc,ck->...rk", values, inverse_columns, precision=HIGHEST) * twiddle
    )
    flattened = partial_value.reshape((-1,) + partial_value.shape[-2:])
    return lax.all_to_all(flattened, "coef", split_axis=2, concat_axis=1, tiled=True)


def to_coefficients(values, twiddle, inverse_rows, inverse_columns):
    leading = values.shape[:-2]
    arrived = columns_section(values, twiddle, inverse_columns)
    output = jnp.einsum("brk,rj->bkj", arrived, inverse_rows, precision=HIGHEST)
    return output.reshape(leading + output.shape[-2:])


def to_values(coeffs, twiddle, forward_rows, forward_columns):
    leading = coeffs.shape[:-2]
    partial_value = jnp.einsum("...cr,rk->...ck", coeffs, forward_rows, precision=HIGHEST) * twiddle
    flattened = partial_value.reshape((-1,) + partial_value.shape[-2:])
    arrived = lax.all_to_all(flattened, "coef", split_axis=2, concat_axis=1, tiled=True)
    output = jnp.einsum("bck,cm->bkm", arrived, forward_columns, precision=HIGHEST)
    return output.reshape(leading + output.shape[-2:])


def general(
    cipher_zero,
    cipher_one,
    key_main,
    key_special,
    lift_main,
    lift_special,
    lower_table,
    inverse_scale,
    inverse_main,
    inverse_special,
    forward_main,
    forward_special,
    inverse_rows,
    inverse_columns,
    forward_rows,
    forward_columns,
):
    ciphers, local_main, positions = cipher_one.shape
    local_special = key_special.shape[3]
    digits = key_main.shape[1]
    rows_here = inverse_main.shape[1]
    cols_here = forward_main.shape[1]
    total_main = lift_main.shape[0]
    limb_index = lax.axis_index("limb")
    owner = (jnp.arange(total_main) // K)[None, :] == jnp.arange(digits)[:, None]
    digit_mask = owner.astype(lift_main.dtype)
    masked_main = digit_mask[:, :, None] * lift_main[None]
    masked_special = digit_mask[:, :, None] * lift_special[None]
    twiddle_both = jnp.concatenate([forward_main, forward_special], axis=0)
    shaped = cipher_one.reshape(ciphers, local_main, rows_here, COLS)
    coeffs = to_coefficients(shaped, inverse_main, inverse_rows, inverse_columns).reshape(
        ciphers, local_main, positions
    )
    own_main = lax.dynamic_slice_in_dim(masked_main, limb_index * local_main, local_main, 2)
    own_special = lax.dynamic_slice_in_dim(
        masked_special, limb_index * local_special, local_special, 2
    )
    portion = lax.all_gather(coeffs, "limb", axis=1, tiled=True)
    lifted_main = jnp.einsum("bsn,dst->bdtn", portion, own_main, precision=HIGHEST)
    lifted_sp = jnp.einsum("bsn,dst->bdtn", portion, own_special, precision=HIGHEST)
    joined = jnp.concatenate([lifted_main, lifted_sp], axis=2)
    joined = joined.reshape(ciphers, digits, local_main + local_special, cols_here, ROWS)
    values_all = to_values(joined, twiddle_both, forward_rows, forward_columns)
    values_all = values_all.reshape(ciphers, digits, local_main + local_special, positions)
    values_main = values_all[:, :, :local_main]
    values_sp = values_all[:, :, local_main:]
    summed_main = jnp.sum(values_main[:, :, None] * key_main.astype(jnp.float32), axis=1)
    summed_sp = jnp.sum(values_sp[:, :, None] * key_special.astype(jnp.float32), axis=1)
    shaped_sp = summed_sp.reshape(ciphers, 2, local_special, rows_here, COLS)
    special = to_coefficients(shaped_sp, inverse_special, inverse_rows, inverse_columns)
    special = special.reshape(ciphers, 2, local_special, positions)
    own_lower = lax.dynamic_slice_in_dim(lower_table, limb_index * local_main, local_main, 1)
    lowered = jnp.einsum(
        "bsjn,jt->bstn",
        lax.all_gather(special, "limb", axis=2, tiled=True),
        own_lower,
        precision=HIGHEST,
    )
    lowered = to_values(
        lowered.reshape(ciphers, 2, local_main, cols_here, ROWS),
        forward_main,
        forward_rows,
        forward_columns,
    )
    lowered = lowered.reshape(ciphers, 2, local_main, positions)
    result = inverse_scale[:, None] * (summed_main - lowered)
    return (cipher_zero + result[:, 0], result[:, 1])


def halves(x):
    high = lax.reduce_precision(x, 8, 7)
    return high.astype(BF16), (x - high).astype(BF16)


def split(x):
    high = x.astype(BF16)
    return high, (x - high.astype(F32)).astype(BF16)


def mm(a, b):
    return jnp.dot(a, b, preferred_element_type=F32)


def mm3(a, b):
    return mm(a[0], b[0]) + (mm(a[1], b[0]) + mm(a[0], b[1]))


def put(scr, x, start=0):
    half = scr.shape[2]
    for h in range(scr.shape[0]):
        scr[h, pl.ds(start, x.shape[0]), :] = x[:, h * half : (h + 1) * half]


def first_kernel(x, tw, wh, wl, out, scr, *, rows, cols):
    limbs = x.shape[1]
    stacked = jnp.concatenate([x[0, :, r * cols : (r + 1) * cols] for r in range(rows)], axis=0)
    put(scr, mm3(split(stacked), (wh[...], wl[...])) * tw[...])
    half = scr.shape[2]
    for d in range(limbs):
        for h in range(scr.shape[0]):
            out[d, 0, :, h * half : (h + 1) * half] = scr[h, pl.ds(d, rows, stride=limbs), :]


def middle_kernel(x, mh, ml, out):
    n, _, rows, cols = x.shape
    y = mm3((mh[...], ml[...]), split(x[...].reshape(n * rows, cols)))
    out[...] = y.reshape(n, 1, rows, cols)


GROUP = 4
TILE = 16


def lift(emit, groups, coef, refs, rows):
    def body(g, carry):
        for row in range(0, rows, TILE):
            sums = [None] * GROUP
            for k, (ref, s) in enumerate(refs):
                poly = ref[s, 0, row : row + TILE, :]
                for j in range(GROUP):
                    add = coef(g * GROUP + j, k) * poly
                    sums[j] = add if sums[j] is None else sums[j] + add
            for j in range(GROUP):
                emit(g * GROUP + j, row, sums[j])
        return carry

    lax.fori_loop(0, groups, body, 0)


def key_kernel(coef, polys, fw, ch, cl, ih, il, tws, km, ks, out, summed, vh, vl, wv, xs, ys):
    both, rows, cols = fw.shape
    digits, main = km.shape[1], km.shape[3]
    special = ks.shape[3]
    lanes, _, half = wv.shape
    span = polys.shape[0] // digits

    for d in range(digits):

        def emit(t, row, value, d=d):
            high, low = split(value * fw[t, row : row + TILE, :])
            at = pl.multiple_of((d * both + t) * rows + row, TILE)
            vh[pl.ds(at, TILE), :] = high
            vl[pl.ds(at, TILE), :] = low

        lift(
            emit,
            both // GROUP,
            lambda t, k, d=d: coef[d, t, k],
            [(polys, d * span + s) for s in range(span)],
            rows,
        )

    put(wv, mm3((vh[...], vl[...]), (ch[...], cl[...])))

    def keys(r, carry):
        for h in range(lanes):
            at = pl.multiple_of(r * cols + h * half, half)
            for keyed, base, count in ((km, 0, main), (ks, main, special)):
                values = [
                    wv[h, pl.ds((d * both + base) * rows + r, count, stride=rows), :]
                    for d in range(digits)
                ]
                for i in range(2):
                    total = None
                    for d in range(digits):
                        add = values[d] * keyed[0, d, i, :, pl.ds(at, half)].astype(F32)
                        total = add if total is None else total + add
                    if base == 0:
                        summed[0, i, :, pl.ds(at, half)] = total
                    else:
                        xs[i, r, :, h * half : (h + 1) * half] = total
        return carry

    lax.fori_loop(0, rows, keys, 0, unroll=4)
    size = rows * special
    y = mm3(split(xs[...].reshape(2 * size, cols)), (ih[...], il[...]))
    for i in range(2):
        put(ys, y[i * size : (i + 1) * size] * tws[...], i * size)
    for i in range(2):
        for u in range(special):
            for h in range(lanes):
                out[i * special + u, 0, :, h * half : (h + 1) * half] = ys[
                    h, pl.ds(i * size + u, rows, stride=special), :
                ]


def end_lower_kernel(coef, *refs):
    ins, out = refs[:-1], refs[-1]
    u = ins[0].shape[0] // 2
    per, rows = out.shape[0] // 2, out.shape[2]
    for i in range(2):

        def emit(t, row, value, i=i):
            out[i * per + t, 0, row : row + TILE, :] = value

        lift(
            emit,
            per // GROUP,
            lambda t, k: coef[t, k],
            [(ref, i * u + s) for ref in ins for s in range(u)],
            rows,
        )


def last_kernel(coef, own, mate, cross, far, ready, fw, ch, cl, scale, summed, zero, *rest):
    out0, out1, done, vh, vl, wv = rest[-6:]
    done[...] = jnp.zeros(done.shape, F32)
    per, rows, cols = fw.shape
    u = own.shape[0] // 2
    lanes, _, half = wv.shape
    for i in range(2):

        def emit(t, row, value, i=i):
            value = value + ready[i * per + t, 0, row : row + TILE, :]
            high, low = split(value * fw[t, row : row + TILE, :])
            at = pl.multiple_of((i * per + t) * rows + row, TILE)
            vh[pl.ds(at, TILE), :] = high
            vl[pl.ds(at, TILE), :] = low

        lift(
            emit,
            per // GROUP,
            lambda t, k: coef[t, k],
            [(ref, i * u + s) for ref in (own, mate, cross, far) for s in range(u)],
            rows,
        )
    put(wv, mm3((vh[...], vl[...]), (ch[...], cl[...])))
    factor = jnp.broadcast_to(scale[...], (per, half))

    def finish(r, carry):
        for h in range(lanes):
            at = pl.multiple_of(r * cols + h * half, half)
            for i, out in enumerate((out0, out1)):
                low = wv[h, pl.ds(i * per * rows + r, per, stride=rows), :]
                value = factor * (summed[0, i, :, pl.ds(at, half)] - low)
                if i == 0:
                    value = zero[0, :, pl.ds(at, half)] + value
                out[0, :, pl.ds(at, half)] = value
        return carry

    lax.fori_loop(0, rows, finish, 0, unroll=4)


def fast(
    cipher_zero,
    cipher_one,
    key_main,
    key_special,
    lift_main,
    lift_special,
    lower_table,
    inverse_scale,
    inverse_main,
    inverse_special,
    forward_main,
    forward_special,
    inverse_rows,
    inverse_columns,
    forward_rows,
    forward_columns,
):
    ciphers, main, positions = cipher_one.shape
    digits = key_main.shape[1]
    special = key_special.shape[3]
    rows, cols = inverse_main.shape[1:]
    n = main
    half = min(cols, 128)
    lanes = cols // half
    both = main + special
    z = lax.axis_index("limb")
    inner = jnp.logical_or(z == 1, z == 2).astype(F32)

    merged = halves(jnp.einsum("rj,jk->kr", inverse_rows, forward_rows, precision=HIGHEST))
    ic = halves(inverse_columns)
    fc = halves(forward_columns)
    tw_in = inverse_main.transpose(1, 0, 2).reshape(rows * main, cols)
    tw_sp = inverse_special.transpose(1, 0, 2).reshape(rows * special, cols)
    fw = jnp.concatenate([forward_main, forward_special], axis=0)
    fw = fw.transpose(2, 0, 1).reshape(n, rows * both * rows // cols, cols)
    fw = lax.all_to_all(fw, "coef", split_axis=0, concat_axis=0)
    fw = fw.reshape(n, rows, both, rows).transpose(2, 1, 0, 3).reshape(both, rows, cols)
    fw_main = fw[:main]

    def columns(full, target, count):
        return lax.dynamic_slice_in_dim(full, target * count, count, 1).T

    def lower_from(source, target):
        full = lax.dynamic_slice_in_dim(lower_table, source * special, special, 0)
        return columns(full, target, main)

    coef_lift = jnp.concatenate(
        [columns(lift_main, z, main), columns(lift_special, z, special)], axis=0
    )
    coef_lift = coef_lift.reshape(both, digits, K).transpose(1, 0, 2)
    mate_z = z ^ 1
    cross_z = 3 - z
    far_z = cross_z ^ 1
    coef_low = jnp.concatenate(
        [lower_from(z, z)]
        + [inner * lower_from(source, z) for source in (mate_z, cross_z, far_z)],
        axis=1,
    )
    coef_low_end = jnp.concatenate(
        [lower_from(source, mate_z) for source in (z, cross_z, far_z)], axis=1
    )
    scale = inverse_scale[:, None]

    smem = pl.BlockSpec(memory_space=pltpu.SMEM)

    def whole(x):
        return pl.BlockSpec(x.shape, lambda c: (0,) * x.ndim)

    def polys(count):
        return pl.BlockSpec((count, 1, rows, cols), lambda c: (0, c, 0, 0))

    def stacked(count, size):
        return jax.ShapeDtypeStruct((count, size, rows, cols), F32)

    def call(kernel, size, in_specs, out_specs, out_shape, scratch, flops, **kw):
        def after(_, *refs):
            kernel(*refs)

        return pl.pallas_call(
            after,
            grid=(size,),
            in_specs=[pl.BlockSpec(memory_space=pl.ANY)] + in_specs,
            out_specs=out_specs,
            scratch_shapes=scratch,
            out_shape=out_shape,
            compiler_params=pltpu.CompilerParams(
                dimension_semantics=("arbitrary",), vmem_limit_bytes=40 * 1024 * 1024
            ),
            cost_estimate=pl.CostEstimate(
                flops=int(flops * size), transcendentals=0, bytes_accessed=0
            ),
            **kw,
        )

    def first(start, size):
        return call(
            functools.partial(first_kernel, rows=rows, cols=cols),
            size,
            [
                pl.BlockSpec((1, main, positions), lambda c: (start + c, 0, 0)),
                whole(tw_in),
                whole(ic[0]),
                whole(ic[1]),
            ],
            polys(n),
            stacked(n, size),
            [pltpu.VMEM((lanes, rows * main, half), F32)],
            1e6,
        )

    def middle(size):
        return call(
            middle_kernel,
            size,
            [polys(n), whole(merged[0]), whole(merged[1])],
            polys(n),
            stacked(n, size),
            [],
            1e6,
        )

    def keyed(start, size):
        return call(
            key_kernel,
            size,
            [smem, polys(digits * K)]
            + [whole(x) for x in (fw, *fc, *ic, tw_sp)]
            + [
                pl.BlockSpec((1, digits, 2, main, positions), lambda c: (start + c, 0, 0, 0, 0)),
                pl.BlockSpec((1, digits, 2, special, positions), lambda c: (start + c, 0, 0, 0, 0)),
            ],
            [polys(n), pl.BlockSpec((1, 2, main, positions), lambda c: (c, 0, 0, 0))],
            [stacked(n, size), jax.ShapeDtypeStruct((size, 2, main, positions), F32)],
            [
                pltpu.VMEM((digits * both * rows, cols), BF16),
                pltpu.VMEM((digits * both * rows, cols), BF16),
                pltpu.VMEM((lanes, digits * both * rows, half), F32),
                pltpu.VMEM((2, rows, special, cols), F32),
                pltpu.VMEM((lanes, 2 * rows * special, half), F32),
            ],
            4e6,
        )

    def end_lower(size):
        return call(
            end_lower_kernel,
            size,
            [smem] + [polys(n)] * 3,
            polys(2 * main),
            stacked(2 * main, size),
            [],
            1e6,
        )

    def last(outs, start, size):
        block = pl.BlockSpec((1, main, positions), lambda c: (start + c, 0, 0))
        kw = {} if outs is None else {"input_output_aliases": {13: 0, 14: 1}}
        return call(
            last_kernel,
            size,
            [smem]
            + [polys(n)] * 4
            + [polys(2 * main)]
            + [whole(x) for x in (fw_main, *fc, scale)]
            + [pl.BlockSpec((1, 2, main, positions), lambda c: (c, 0, 0, 0)), block]
            + ([] if outs is None else [pl.BlockSpec(memory_space=pl.ANY)] * 2),
            [block, block, pl.BlockSpec((8, half), lambda c: (0, 0))],
            [jax.ShapeDtypeStruct(cipher_zero.shape, F32)] * 2
            + [jax.ShapeDtypeStruct((8, half), F32)],
            [
                pltpu.VMEM((2 * main * rows, cols), BF16),
                pltpu.VMEM((2 * main * rows, cols), BF16),
                pltpu.VMEM((lanes, 2 * main * rows, half), F32),
            ],
            3e6,
            **kw,
        )

    def exchange(x):
        return lax.all_to_all(x, "coef", split_axis=0, concat_axis=0, tiled=True)

    def inward(x):
        return lax.ppermute(x, "limb", [(0, 1), (3, 2)])

    def across(x):
        return lax.ppermute(x, "limb", [(1, 2), (2, 1)])

    def outward(x):
        return lax.ppermute(x, "limb", [(1, 0), (2, 3)])

    chunks = []
    at = 0
    for size in SIZES if sum(SIZES) == ciphers else [1] * ciphers:
        chunks.append((at, size))
        at += size

    state = [{} for _ in chunks]
    token = tw_in
    outs = None
    for c, stage in schedule(len(chunks)):
        start, size = chunks[c]
        st = state[c]

        if stage == "A":
            token = y = first(start, size)(token, cipher_one, tw_in, *ic)
        elif stage in "BE":
            token = y = middle(size)(token, st["x"], *merged)
        elif stage == "D":
            y, st["summed"] = keyed(start, size)(
                token, coef_lift, st["x"], fw, *fc, *ic, tw_sp, key_main, key_special
            )
            token = y
        elif stage == "F":
            own, mate, cross, far = st["x"]
            token = y = end_lower(size)(token, coef_low_end, own, cross, far)
        else:
            extra = () if outs is None else outs
            *outs, token = last(outs, start, size)(
                token,
                coef_low,
                *st["x"],
                st["ready"],
                fw_main,
                *fc,
                scale,
                st["summed"],
                cipher_zero,
                *extra,
            )
        if stage in "ABDE":
            y = exchange(y)
        if stage == "B":
            y = lax.all_gather(y, "limb", axis=0, tiled=True)
        if stage == "E":
            own = y
            mate = inward(own)
            cross = across(own)
            far = across(mate)
            y = (own, mate, cross, far)
        if stage == "F":
            st["ready"] = outward(y)
        else:
            st["x"] = y
    return tuple(outs)


def schedule(n):
    order = [(0, "A"), (0, "B"), (1, "A"), (1, "B")]
    for s in range(n - 1):
        order += [(s, "D"), (s + 2, "A"), (s, "E"), (s - 1, "F"), (s + 2, "B"), (s - 2, "G")]
    s = n - 1
    order += [(s, "D"), (s - 1, "F"), (s, "E"), (s - 2, "G"), (s - 1, "G"), (s, "F"), (s, "G")]
    return [(c, stage) for c, stage in order if 0 <= c < n]


def solution(mesh):
    placed = (
        P(None, "limb", "coef"),
        P(None, "limb", "coef"),
        P(None, None, None, "limb", "coef"),
        P(None, None, None, "limb", "coef"),
        P(),
        P(),
        P(),
        P("limb"),
        P("limb", "coef", None),
        P("limb", "coef", None),
        P("limb", "coef", None),
        P("limb", "coef", None),
        P(),
        P(),
        P(),
        P(),
    )
    limb = mesh.shape["limb"]
    coef = mesh.shape["coef"]

    def on_device(*args):
        main = args[1].shape[1]
        special = args[3].shape[3]
        digits = args[2].shape[1]
        suits = (
            limb == 4
            and digits == 2
            and main == 8
            and special == 4
            and coef == main
            and 2 * K == limb * main
            and args[8].shape[1] * coef == ROWS == COLS
        )
        if suits:
            return fast(*args)
        return general(*args)

    return jax.shard_map(
        on_device,
        mesh=mesh,
        in_specs=placed,
        out_specs=(P(None, "limb", "coef"), P(None, "limb", "coef")),
        check_vma=False,
    )
```

```python
import functools

import jax
import jax.numpy as jnp
from jax import lax
from jax.experimental import pallas as pl
from jax.experimental.pallas import tpu as pltpu
from jax.sharding import PartitionSpec as P


K = 16
ROWS = 256
COLS = 256
SIZES = (2, 4, 4, 4, 4, 4, 2)
PER = 2
F32 = jnp.float32
BF16 = jnp.bfloat16


HIGHEST = lax.Precision.HIGHEST


def columns_section(values, twiddle, inverse_columns):
    partial_value = (
        jnp.einsum("...rc,ck->...rk", values, inverse_columns, precision=HIGHEST) * twiddle
    )
    flattened = partial_value.reshape((-1,) + partial_value.shape[-2:])
    return lax.all_to_all(flattened, "coef", split_axis=2, concat_axis=1, tiled=True)


def to_coefficients(values, twiddle, inverse_rows, inverse_columns):
    leading = values.shape[:-2]
    arrived = columns_section(values, twiddle, inverse_columns)
    output = jnp.einsum("brk,rj->bkj", arrived, inverse_rows, precision=HIGHEST)
    return output.reshape(leading + output.shape[-2:])


def to_values(coeffs, twiddle, forward_rows, forward_columns):
    leading = coeffs.shape[:-2]
    partial_value = jnp.einsum("...cr,rk->...ck", coeffs, forward_rows, precision=HIGHEST) * twiddle
    flattened = partial_value.reshape((-1,) + partial_value.shape[-2:])
    arrived = lax.all_to_all(flattened, "coef", split_axis=2, concat_axis=1, tiled=True)
    output = jnp.einsum("bck,cm->bkm", arrived, forward_columns, precision=HIGHEST)
    return output.reshape(leading + output.shape[-2:])


def general(
    cipher_zero,
    cipher_one,
    key_main,
    key_special,
    lift_main,
    lift_special,
    lower_table,
    inverse_scale,
    inverse_main,
    inverse_special,
    forward_main,
    forward_special,
    inverse_rows,
    inverse_columns,
    forward_rows,
    forward_columns,
):
    ciphers, local_main, positions = cipher_one.shape
    local_special = key_special.shape[3]
    digits = key_main.shape[1]
    rows_here = inverse_main.shape[1]
    cols_here = forward_main.shape[1]
    total_main = lift_main.shape[0]
    limb_index = lax.axis_index("limb")
    owner = (jnp.arange(total_main) // K)[None, :] == jnp.arange(digits)[:, None]
    digit_mask = owner.astype(lift_main.dtype)
    masked_main = digit_mask[:, :, None] * lift_main[None]
    masked_special = digit_mask[:, :, None] * lift_special[None]
    twiddle_both = jnp.concatenate([forward_main, forward_special], axis=0)
    shaped = cipher_one.reshape(ciphers, local_main, rows_here, COLS)
    coeffs = to_coefficients(shaped, inverse_main, inverse_rows, inverse_columns).reshape(
        ciphers, local_main, positions
    )
    own_main = lax.dynamic_slice_in_dim(masked_main, limb_index * local_main, local_main, 2)
    own_special = lax.dynamic_slice_in_dim(
        masked_special, limb_index * local_special, local_special, 2
    )
    portion = lax.all_gather(coeffs, "limb", axis=1, tiled=True)
    lifted_main = jnp.einsum("bsn,dst->bdtn", portion, own_main, precision=HIGHEST)
    lifted_sp = jnp.einsum("bsn,dst->bdtn", portion, own_special, precision=HIGHEST)
    joined = jnp.concatenate([lifted_main, lifted_sp], axis=2)
    joined = joined.reshape(ciphers, digits, local_main + local_special, cols_here, ROWS)
    values_all = to_values(joined, twiddle_both, forward_rows, forward_columns)
    values_all = values_all.reshape(ciphers, digits, local_main + local_special, positions)
    values_main = values_all[:, :, :local_main]
    values_sp = values_all[:, :, local_main:]
    summed_main = jnp.sum(values_main[:, :, None] * key_main.astype(jnp.float32), axis=1)
    summed_sp = jnp.sum(values_sp[:, :, None] * key_special.astype(jnp.float32), axis=1)
    shaped_sp = summed_sp.reshape(ciphers, 2, local_special, rows_here, COLS)
    special = to_coefficients(shaped_sp, inverse_special, inverse_rows, inverse_columns)
    special = special.reshape(ciphers, 2, local_special, positions)
    own_lower = lax.dynamic_slice_in_dim(lower_table, limb_index * local_main, local_main, 1)
    lowered = jnp.einsum(
        "bsjn,jt->bstn",
        lax.all_gather(special, "limb", axis=2, tiled=True),
        own_lower,
        precision=HIGHEST,
    )
    lowered = to_values(
        lowered.reshape(ciphers, 2, local_main, cols_here, ROWS),
        forward_main,
        forward_rows,
        forward_columns,
    )
    lowered = lowered.reshape(ciphers, 2, local_main, positions)
    result = inverse_scale[:, None] * (summed_main - lowered)
    return (cipher_zero + result[:, 0], result[:, 1])


def halves(x):
    high = lax.reduce_precision(x, 8, 7)
    return high.astype(BF16), (x - high).astype(BF16)


def split(x):
    high = x.astype(BF16)
    return high, (x - high.astype(F32)).astype(BF16)


def mm(a, b):
    return jnp.dot(a, b, preferred_element_type=F32)


def mm3(a, b):
    return mm(a[0], b[0]) + (mm(a[1], b[0]) + mm(a[0], b[1]))


def put(scr, x, start=0):
    half = scr.shape[2]
    for h in range(scr.shape[0]):
        scr[h, pl.ds(start, x.shape[0]), :] = x[:, h * half : (h + 1) * half]


def first_kernel(x, tw, wh, wl, out, scr, *, rows, cols):
    limbs = x.shape[1]
    half = scr.shape[2]
    for c in range(x.shape[0]):
        stacked = jnp.concatenate(
            [x[c, :, r * cols : (r + 1) * cols] for r in range(rows)], axis=0
        )
        put(scr, mm3(split(stacked), (wh[...], wl[...])) * tw[...])
        for d in range(limbs):
            for h in range(scr.shape[0]):
                out[d, c, :, h * half : (h + 1) * half] = scr[h, pl.ds(d, rows, stride=limbs), :]


def middle_kernel(x, mh, ml, out):
    n, cts, rows, cols = x.shape
    for c in range(cts):
        y = mm3((mh[...], ml[...]), split(x[:, c].reshape(n * rows, cols)))
        out[:, c] = y.reshape(n, rows, cols)


GROUP = 4
TILE = 16


def lift(emit, groups, coef, refs, rows):
    def body(g, carry):
        for row in range(0, rows, TILE):
            sums = [None] * GROUP
            for k, (ref, s) in enumerate(refs):
                poly = ref[s, 0, row : row + TILE, :]
                for j in range(GROUP):
                    add = coef(g * GROUP + j, k) * poly
                    sums[j] = add if sums[j] is None else sums[j] + add
            for j in range(GROUP):
                emit(g * GROUP + j, row, sums[j])
        return carry

    lax.fori_loop(0, groups, body, 0)


def key_kernel(coef, polys, fw, ch, cl, ih, il, tws, km, ks, out, summed, vh, vl, wv, xs, ys):
    both, rows, cols = fw.shape
    digits, main = km.shape[1], km.shape[3]
    special = ks.shape[3]
    lanes, _, half = wv.shape
    span = polys.shape[0] // digits

    for d in range(digits):

        def emit(t, row, value, d=d):
            high, low = split(value * fw[t, row : row + TILE, :])
            at = pl.multiple_of((d * both + t) * rows + row, TILE)
            vh[pl.ds(at, TILE), :] = high
            vl[pl.ds(at, TILE), :] = low

        lift(
            emit,
            both // GROUP,
            lambda t, k, d=d: coef[d, t, k],
            [(polys, d * span + s) for s in range(span)],
            rows,
        )

    put(wv, mm3((vh[...], vl[...]), (ch[...], cl[...])))

    def keys(r, carry):
        for h in range(lanes):
            at = pl.multiple_of(r * cols + h * half, half)
            for keyed, base, count in ((km, 0, main), (ks, main, special)):
                values = [
                    wv[h, pl.ds((d * both + base) * rows + r, count, stride=rows), :]
                    for d in range(digits)
                ]
                for i in range(2):
                    total = None
                    for d in range(digits):
                        add = values[d] * keyed[0, d, i, :, pl.ds(at, half)].astype(F32)
                        total = add if total is None else total + add
                    if base == 0:
                        summed[0, i, :, pl.ds(at, half)] = total
                    else:
                        xs[i, r, :, h * half : (h + 1) * half] = total
        return carry

    lax.fori_loop(0, rows, keys, 0, unroll=4)
    size = rows * special
    y = mm3(split(xs[...].reshape(2 * size, cols)), (ih[...], il[...]))
    for i in range(2):
        put(ys, y[i * size : (i + 1) * size] * tws[...], i * size)
    for i in range(2):
        for u in range(special):
            for h in range(lanes):
                out[i * special + u, 0, :, h * half : (h + 1) * half] = ys[
                    h, pl.ds(i * size + u, rows, stride=special), :
                ]


def end_lower_kernel(coef, *refs):
    ins, out = refs[:-1], refs[-1]
    u = ins[0].shape[0] // 2
    per, rows = out.shape[0] // 2, out.shape[2]
    for i in range(2):

        def emit(t, row, value, i=i):
            out[i * per + t, 0, row : row + TILE, :] = value

        lift(
            emit,
            per // GROUP,
            lambda t, k: coef[t, k],
            [(ref, i * u + s) for ref in ins for s in range(u)],
            rows,
        )


def last_kernel(coef, own, mate, cross, far, ready, fw, ch, cl, scale, summed, zero, *rest):
    out0, out1, done, vh, vl, wv = rest[-6:]
    done[...] = jnp.zeros(done.shape, F32)
    per, rows, cols = fw.shape
    u = own.shape[0] // 2
    lanes, _, half = wv.shape
    for i in range(2):

        def emit(t, row, value, i=i):
            value = value + ready[i * per + t, 0, row : row + TILE, :]
            high, low = split(value * fw[t, row : row + TILE, :])
            at = pl.multiple_of((i * per + t) * rows + row, TILE)
            vh[pl.ds(at, TILE), :] = high
            vl[pl.ds(at, TILE), :] = low

        lift(
            emit,
            per // GROUP,
            lambda t, k: coef[t, k],
            [(ref, i * u + s) for ref in (own, mate, cross, far) for s in range(u)],
            rows,
        )
    put(wv, mm3((vh[...], vl[...]), (ch[...], cl[...])))
    factor = jnp.broadcast_to(scale[...], (per, half))

    def finish(r, carry):
        for h in range(lanes):
            at = pl.multiple_of(r * cols + h * half, half)
            for i, out in enumerate((out0, out1)):
                low = wv[h, pl.ds(i * per * rows + r, per, stride=rows), :]
                value = factor * (summed[0, i, :, pl.ds(at, half)] - low)
                if i == 0:
                    value = zero[0, :, pl.ds(at, half)] + value
                out[0, :, pl.ds(at, half)] = value
        return carry

    lax.fori_loop(0, rows, finish, 0, unroll=4)


def fast(
    cipher_zero,
    cipher_one,
    key_main,
    key_special,
    lift_main,
    lift_special,
    lower_table,
    inverse_scale,
    inverse_main,
    inverse_special,
    forward_main,
    forward_special,
    inverse_rows,
    inverse_columns,
    forward_rows,
    forward_columns,
):
    ciphers, main, positions = cipher_one.shape
    digits = key_main.shape[1]
    special = key_special.shape[3]
    rows, cols = inverse_main.shape[1:]
    n = main
    half = min(cols, 128)
    lanes = cols // half
    both = main + special
    z = lax.axis_index("limb")
    inner = jnp.logical_or(z == 1, z == 2).astype(F32)

    merged = halves(jnp.einsum("rj,jk->kr", inverse_rows, forward_rows, precision=HIGHEST))
    ic = halves(inverse_columns)
    fc = halves(forward_columns)
    tw_in = inverse_main.transpose(1, 0, 2).reshape(rows * main, cols)
    tw_sp = inverse_special.transpose(1, 0, 2).reshape(rows * special, cols)
    fw = jnp.concatenate([forward_main, forward_special], axis=0)
    fw = fw.transpose(2, 0, 1).reshape(n, rows * both * rows // cols, cols)
    fw = lax.all_to_all(fw, "coef", split_axis=0, concat_axis=0)
    fw = fw.reshape(n, rows, both, rows).transpose(2, 1, 0, 3).reshape(both, rows, cols)
    fw_main = fw[:main]

    def columns(full, target, count):
        return lax.dynamic_slice_in_dim(full, target * count, count, 1).T

    def lower_from(source, target):
        full = lax.dynamic_slice_in_dim(lower_table, source * special, special, 0)
        return columns(full, target, main)

    coef_lift = jnp.concatenate(
        [columns(lift_main, z, main), columns(lift_special, z, special)], axis=0
    )
    coef_lift = coef_lift.reshape(both, digits, K).transpose(1, 0, 2)
    mate_z = z ^ 1
    cross_z = 3 - z
    far_z = cross_z ^ 1
    coef_low = jnp.concatenate(
        [lower_from(z, z)]
        + [inner * lower_from(source, z) for source in (mate_z, cross_z, far_z)],
        axis=1,
    )
    coef_low_end = jnp.concatenate(
        [lower_from(source, mate_z) for source in (z, cross_z, far_z)], axis=1
    )
    scale = inverse_scale[:, None]

    smem = pl.BlockSpec(memory_space=pltpu.SMEM)

    def whole(x):
        return pl.BlockSpec(x.shape, lambda c: (0,) * x.ndim)

    def polys(count, cts=1):
        return pl.BlockSpec((count, cts, rows, cols), lambda c: (0, c, 0, 0))

    def stacked(count, size):
        return jax.ShapeDtypeStruct((count, size, rows, cols), F32)

    def call(kernel, size, in_specs, out_specs, out_shape, scratch, flops, **kw):
        def after(_, *refs):
            kernel(*refs)

        return pl.pallas_call(
            after,
            grid=(size,),
            in_specs=[pl.BlockSpec(memory_space=pl.ANY)] + in_specs,
            out_specs=out_specs,
            scratch_shapes=scratch,
            out_shape=out_shape,
            compiler_params=pltpu.CompilerParams(
                dimension_semantics=("arbitrary",), vmem_limit_bytes=60 * 1024 * 1024
            ),
            cost_estimate=pl.CostEstimate(
                flops=int(flops * size), transcendentals=0, bytes_accessed=0
            ),
            **kw,
        )

    def first(start, size):
        per = PER if start % PER == 0 and size % PER == 0 else 1
        return call(
            functools.partial(first_kernel, rows=rows, cols=cols),
            size // per,
            [
                pl.BlockSpec((per, main, positions), lambda c: (start // per + c, 0, 0)),
                whole(tw_in),
                whole(ic[0]),
                whole(ic[1]),
            ],
            polys(n, per),
            stacked(n, size),
            [pltpu.VMEM((lanes, rows * main, half), F32)],
            2e6,
        )

    def middle(size):
        per = PER if size % PER == 0 else 1
        return call(
            middle_kernel,
            size // per,
            [polys(n, per), whole(merged[0]), whole(merged[1])],
            polys(n, per),
            stacked(n, size),
            [],
            1e6,
        )

    def keyed(start, size):
        return call(
            key_kernel,
            size,
            [smem, polys(digits * K)]
            + [whole(x) for x in (fw, *fc, *ic, tw_sp)]
            + [
                pl.BlockSpec((1, digits, 2, main, positions), lambda c: (start + c, 0, 0, 0, 0)),
                pl.BlockSpec((1, digits, 2, special, positions), lambda c: (start + c, 0, 0, 0, 0)),
            ],
            [polys(n), pl.BlockSpec((1, 2, main, positions), lambda c: (c, 0, 0, 0))],
            [stacked(n, size), jax.ShapeDtypeStruct((size, 2, main, positions), F32)],
            [
                pltpu.VMEM((digits * both * rows, cols), BF16),
                pltpu.VMEM((digits * both * rows, cols), BF16),
                pltpu.VMEM((lanes, digits * both * rows, half), F32),
                pltpu.VMEM((2, rows, special, cols), F32),
                pltpu.VMEM((lanes, 2 * rows * special, half), F32),
            ],
            4e6,
        )

    def end_lower(size):
        return call(
            end_lower_kernel,
            size,
            [smem] + [polys(n)] * 3,
            polys(2 * main),
            stacked(2 * main, size),
            [],
            1e6,
        )

    def last(outs, start, size):
        block = pl.BlockSpec((1, main, positions), lambda c: (start + c, 0, 0))
        kw = {} if outs is None else {"input_output_aliases": {13: 0, 14: 1}}
        return call(
            last_kernel,
            size,
            [smem]
            + [polys(n)] * 4
            + [polys(2 * main)]
            + [whole(x) for x in (fw_main, *fc, scale)]
            + [pl.BlockSpec((1, 2, main, positions), lambda c: (c, 0, 0, 0)), block]
            + ([] if outs is None else [pl.BlockSpec(memory_space=pl.ANY)] * 2),
            [block, block, pl.BlockSpec((8, half), lambda c: (0, 0))],
            [jax.ShapeDtypeStruct(cipher_zero.shape, F32)] * 2
            + [jax.ShapeDtypeStruct((8, half), F32)],
            [
                pltpu.VMEM((2 * main * rows, cols), BF16),
                pltpu.VMEM((2 * main * rows, cols), BF16),
                pltpu.VMEM((lanes, 2 * main * rows, half), F32),
            ],
            3e6,
            **kw,
        )

    def exchange(x):
        return lax.all_to_all(x, "coef", split_axis=0, concat_axis=0, tiled=True)

    def inward(x):
        return lax.ppermute(x, "limb", [(0, 1), (3, 2)])

    def across(x):
        return lax.ppermute(x, "limb", [(1, 2), (2, 1)])

    def outward(x):
        return lax.ppermute(x, "limb", [(1, 0), (2, 3)])

    chunks = []
    at = 0
    for size in SIZES if sum(SIZES) == ciphers else [1] * ciphers:
        chunks.append((at, size))
        at += size

    state = [{} for _ in chunks]
    token = tw_in
    outs = None
    for c, stage in schedule(len(chunks)):
        start, size = chunks[c]
        st = state[c]

        if stage == "A":
            token = y = first(start, size)(token, cipher_one, tw_in, *ic)
        elif stage in "BE":
            token = y = middle(size)(token, st["x"], *merged)
        elif stage == "D":
            y, st["summed"] = keyed(start, size)(
                token, coef_lift, st["x"], fw, *fc, *ic, tw_sp, key_main, key_special
            )
            token = y
        elif stage == "F":
            own, mate, cross, far = st["x"]
            token = y = end_lower(size)(token, coef_low_end, own, cross, far)
        else:
            extra = () if outs is None else outs
            *outs, token = last(outs, start, size)(
                token,
                coef_low,
                *st["x"],
                st["ready"],
                fw_main,
                *fc,
                scale,
                st["summed"],
                cipher_zero,
                *extra,
            )
        if stage in "ABDE":
            y = exchange(y)
        if stage == "B":
            y = lax.all_gather(y, "limb", axis=0, tiled=True)
        if stage == "E":
            own = y
            mate = inward(own)
            cross = across(own)
            far = across(mate)
            y = (own, mate, cross, far)
        if stage == "F":
            st["ready"] = outward(y)
        else:
            st["x"] = y
    return tuple(outs)


AHEAD = 3


def schedule(n):
    order = [(c, stage) for c in range(AHEAD) for stage in "AB"]
    for s in range(n - 1):
        order += [(s, "D"), (s + AHEAD, "A"), (s, "E"), (s - 3, "G"), (s - 1, "F")]
        order += [(s + AHEAD, "B")]
    s = n - 1
    order += [(s, "D"), (s - 1, "F"), (s, "E"), (s - 3, "G"), (s - 2, "G"), (s, "F")]
    order += [(s - 1, "G"), (s, "G")]
    return [(c, stage) for c, stage in order if 0 <= c < n]


def solution(mesh):
    placed = (
        P(None, "limb", "coef"),
        P(None, "limb", "coef"),
        P(None, None, None, "limb", "coef"),
        P(None, None, None, "limb", "coef"),
        P(),
        P(),
        P(),
        P("limb"),
        P("limb", "coef", None),
        P("limb", "coef", None),
        P("limb", "coef", None),
        P("limb", "coef", None),
        P(),
        P(),
        P(),
        P(),
    )
    limb = mesh.shape["limb"]
    coef = mesh.shape["coef"]

    def on_device(*args):
        main = args[1].shape[1]
        special = args[3].shape[3]
        digits = args[2].shape[1]
        suits = (
            limb == 4
            and digits == 2
            and main == 8
            and special == 4
            and coef == main
            and 2 * K == limb * main
            and args[8].shape[1] * coef == ROWS == COLS
        )
        if suits:
            return fast(*args)
        return general(*args)

    return jax.shard_map(
        on_device,
        mesh=mesh,
        in_specs=placed,
        out_specs=(P(None, "limb", "coef"), P(None, "limb", "coef")),
        check_vma=False,
    )
```
